32 devices in a mesh: groups: 2 (over y), expert: 8 (over z, x), tensor: 2 (over core).
Axes of the slice: x: 2, y: 2, z: 4, core: 2. Of those that a mesh axis runs over, the one named last changes fastest.
Arguments:
- tokens: bfloat16 [4096, 1440], P(('groups', 'expert')), parts along dimension 0, may hold values from -6 to 6
- routes: int32 [4096, 4], P(('groups', 'expert')), parts along dimension 0, may hold values from 0 to 7, all different within a row; in each aligned block of 256 rows (0 to 255, 256 to 511, ...) at most 192 rows name the same one
- gates: float32 [4096, 4], P(('groups', 'expert')), parts along dimension 0, may hold values from 0.1 to 1
- w_gate: bfloat16 [8, 1440, 1440], P('expert', None, 'tensor'), may hold values from -0.15625 to 0.15625
- w_up: bfloat16 [8, 1440, 1440], P('expert', None, 'tensor'), may hold values from -0.15625 to 0.15625
- w_down: bfloat16 [8, 1440, 1440], P('expert', 'tensor'), may hold values from -0.15625 to 0.15625
- shared_gate: bfloat16 [1440, 1440], P(None, 'tensor'), may hold values from -0.15625 to 0.15625
- shared_up: bfloat16 [1440, 1440], P(None, 'tensor'), may hold values from -0.15625 to 0.15625
- shared_down: bfloat16 [1440, 1440], P('tensor'), may hold values from -0.15625 to 0.15625
Outputs:
- mixed: bfloat16 [4096, 1440], P(('groups', 'expert'), 'tensor'), parts along dimension 0
The draws below stay inside these ranges and needn't reach their ends.
There are 2 independent parts, one for each index of `groups`. The reference program is written for one: setup_inputs(seed, part) draws one part's arguments, and reference() takes and returns one part's arrays. A program takes and returns all parts, laid end to end along the dimension named above; an argument that names none is the same for every part. Nothing has to cross between parts.
Inputs may be any that keep to these rules, and one draw needn't show every extreme that they name: `routes`: each token names 4 different experts. Among the 256 tokens of one index of expert (aligned blocks of rows), no expert is named by more than 192 tokens; in some blocks one expert is named by exactly 192.
All inputs are finite; a program needn't handle non-finite values.
Results may differ from the reference program's by a relative error of at most 0.0051.
Values may be sent and summed in bfloat16 or wider, within the bound.
A program may use at most 192 MiB of HBM per device.

```python
import math
import jax
import jax.numpy as jnp
import numpy as np
from jax import lax

D = 1440
FF = 1440
FS = 1440
TOP = 4
TOK_DEV = 256
EXPERTS = 8
TOKENS = 2048
CAP = 192
N_EXPERT = 8


def levels(stream_key, dims, cuts, least, high):
    level, own = 1.0, jax.random.fold_in(stream_key, 6)
    for dim, blocks in cuts:
        heights = jnp.exp(jax.random.uniform(jax.random.fold_in(own, dim), (blocks,), jnp.float32, least / len(cuts), high / len(cuts)))
        level = level * jnp.repeat(heights, dims[dim] // blocks).reshape([-1 if axis == dim else 1 for axis in range(len(dims))])
    return level


def deal_out(stream_key, own, number, rows, count, top, bound, slope):
    ranking = jax.random.permutation(stream_key, count)
    crowded, usual = shares(count, rows * top, bound, slope, True), shares(count, rows * top, bound, slope, False)
    places = jnp.arange(count)

    def named(tallies, turn):
        used = int((tallies > 0).sum())
        fixed = max(1, used // 4)
        shifted = fixed + (places - fixed + turn * (used - fixed)) % max(1, count - fixed)
        return jnp.zeros((count,), jnp.int32).at[ranking[jnp.where(places < fixed, places, shifted)]].set(jnp.asarray(tallies, jnp.int32))

    tallies = jnp.where(number % 4 == 0, named(crowded, number // 4), named(usual, number - number // 4 - 1))
    mixed = jax.random.permutation(jax.random.fold_in(own, 3), count)
    source_of, receiver = mixed[0:count // 2 * 2:2], mixed[1:count // 2 * 2:2]
    margin = jnp.minimum(tallies[source_of] - 1, bound - tallies[receiver]) // 2
    margin = jnp.where((source_of == ranking[0]) | (receiver == ranking[0]) | (tallies[receiver] == 0), 0, jnp.maximum(margin, 0))
    shifted = jax.random.randint(jax.random.fold_in(own, 4), (count // 2,), 0, 1 << 20) % (margin + 1)
    tallies = tallies.at[source_of].add(-shifted).at[receiver].add(shifted)
    labels = jnp.searchsorted(jnp.cumsum(tallies), jnp.arange(rows * top), side="right").astype(jnp.int32)
    table = labels.reshape(top, rows).T
    table = table[jax.random.permutation(jax.random.fold_in(own, 1), rows)]
    turn = jax.random.randint(jax.random.fold_in(own, 2), (rows, 1), 0, top)
    return jnp.take_along_axis(table, (jnp.arange(top)[None, :] + turn) % top, axis=1)


def shares(amount, total, most, lean, full):
    loads = [(1 << 20) // math.isqrt(rank ** lean) + 1 for rank in range(1, amount + 1)]
    largest = most if full else min(most, max(-(-total // amount), total * loads[0] // sum(loads)))
    least = 1 if total - largest >= amount - 1 else 0
    holding, spare = [largest] + [least] * (amount - 1), total - largest - least * (amount - 1)
    while spare > 0:
        movable = [i for i in range(1, amount) if holding[i] < largest] or [i for i in range(1, amount) if holding[i] < most]
        whole, budget = sum([loads[i] for i in movable]), spare
        for i in movable:
            more = min(most - holding[i], max(1, budget * loads[i] // whole), spare)
            holding[i] = holding[i] + more
            spare = spare - more
    return np.array(holding)


def scatter_about(stream_key, shape, scale, most, cuts=(), kind=jnp.bfloat16):
    drawn = scale * jax.random.normal(stream_key, shape, jnp.float32)
    if cuts:
        drawn = drawn * levels(stream_key, shape, cuts, -0.22, 0.18)
    return jnp.clip(drawn, -most, most).astype(kind)


def setup_inputs(seed: int = 0, part: int = 0) -> dict:
    key_of = jax.random.split(jax.random.key(seed), 10)
    part_keys = jax.random.split(jax.random.fold_in(key_of[9], part), 10)
    tokens = scatter_about(part_keys[0], (TOKENS, D), 1.0, 6.0, ((0, 8),))
    routes_keys = jax.random.split(jax.random.fold_in(part_keys[1], 1), TOKENS // TOK_DEV)
    routes_turns = jax.random.permutation(jax.random.fold_in(part_keys[1], 3), TOKENS // TOK_DEV)
    routes = jax.vmap(lambda own, number: deal_out(jax.random.fold_in(part_keys[1], 2), own, number, TOK_DEV, EXPERTS, TOP, CAP, 2))(routes_keys, routes_turns).reshape((TOKENS, TOP))
    gates = jnp.clip(0.1 + 0.9 * jax.random.uniform(part_keys[2], (TOKENS, TOP), jnp.float32) ** levels(part_keys[2], (TOKENS, TOP), ((0, 8),), -0.2, 0.2), 0.1, 1.0)
    w_gate = scatter_about(key_of[3], (EXPERTS, D, FF), D ** -0.5, 0.15625, ((0, 8), (2, 2)))
    w_up = scatter_about(key_of[4], (EXPERTS, D, FF), D ** -0.5, 0.15625, ((0, 8), (2, 2)))
    w_down = scatter_about(key_of[5], (EXPERTS, FF, D), FF ** -0.5, 0.15625, ((0, 8), (1, 2)))
    shared_gate = scatter_about(key_of[6], (D, FS), D ** -0.5, 0.15625, ((1, 2),))
    shared_up = scatter_about(key_of[7], (D, FS), D ** -0.5, 0.15625, ((1, 2),))
    shared_down = scatter_about(key_of[8], (FS, D), FS ** -0.5, 0.15625, ((0, 2),))
    return {"tokens": tokens, "routes": routes, "gates": gates, "w_gate": w_gate, "w_up": w_up, "w_down": w_down, "shared_gate": shared_gate, "shared_up": shared_up, "shared_down": shared_down}


def reference(tokens, routes, gates, w_gate, w_up, w_down, shared_gate, shared_up, shared_down):
    blocked = routes.reshape(N_EXPERT, TOK_DEV * TOP)
    onehot = (blocked[:, :, None] == jnp.arange(EXPERTS, dtype=jnp.int32)[None, None, :]).astype(jnp.int32)
    order_in = jnp.sum(jnp.cumsum(onehot, axis=1) * onehot, axis=2) - 1
    source = jnp.arange(N_EXPERT, dtype=jnp.int32)[:, None]
    width_all = N_EXPERT * CAP
    slot_index = (blocked * width_all + source * CAP + order_in).reshape(-1).astype(jnp.int32)
    owner = jnp.repeat(jnp.arange(TOKENS, dtype=jnp.int32), TOP)
    token_of = jnp.full((EXPERTS * width_all,), TOKENS, jnp.int32).at[slot_index].set(owner)
    token_of = token_of.reshape(EXPERTS, width_all)
    padded = jnp.concatenate([tokens, jnp.zeros((1, D), tokens.dtype)], 0)

    def expert_rows(operands):
        index_rows, gate_mat, up_mat, down_mat = operands
        gathered = padded[index_rows]
        gate_val = jnp.dot(gathered, gate_mat, preferred_element_type=jnp.float32)
        up_val = jnp.dot(gathered, up_mat, preferred_element_type=jnp.float32)
        hidden = (jax.nn.silu(gate_val) * up_val).astype(jnp.bfloat16)
        return jnp.dot(hidden, down_mat, preferred_element_type=jnp.float32).astype(jnp.bfloat16)

    outputs = lax.map(expert_rows, (token_of, w_gate, w_up, w_down))
    picked = outputs.reshape(EXPERTS * width_all, D)[slot_index].reshape(TOKENS, TOP, D).astype(jnp.float32)
    routed = jnp.sum(gates[:, :, None] * picked, axis=1)
    shared_g = jnp.dot(tokens, shared_gate, preferred_element_type=jnp.float32)
    shared_u = jnp.dot(tokens, shared_up, preferred_element_type=jnp.float32)
    shared_hidden = (jax.nn.silu(shared_g) * shared_u).astype(jnp.bfloat16)
    shared_out = jnp.dot(shared_hidden, shared_down, preferred_element_type=jnp.float32)
    return (tokens.astype(jnp.float32) + routed + shared_out).astype(jnp.bfloat16)
```

```python
import functools

import jax
import jax.numpy as jnp
from jax import lax
from jax.experimental import pallas as pl
from jax.experimental.pallas import tpu as pltpu
from jax.sharding import PartitionSpec as P

MESH = pl.DeviceIdType.MESH
VMEM_BUDGET = 52 * 1024 * 1024


def exchange_local(tokens, routes, gates, w_gate, w_up, w_down, shared_gate, shared_up, shared_down):
    tok_count, top_count = routes.shape
    width_all = tokens.shape[1]
    local_experts = w_gate.shape[0]
    expert_count = lax.axis_size("expert")
    experts_all = expert_count * local_experts
    capacity = max(2, (3 * tok_count * top_count + 2 * experts_all - 1) // (2 * experts_all))
    flat_routes = routes.reshape(-1)
    onehot = (flat_routes[:, None] == jnp.arange(experts_all, dtype=jnp.int32)[None, :]).astype(
        jnp.int32
    )
    order_in = jnp.sum(jnp.cumsum(onehot, axis=0) * onehot, axis=1) - 1
    slot_index = flat_routes * capacity + order_in
    half_width = width_all // lax.axis_size("tensor")
    own_cols = lax.dynamic_slice_in_dim(
        tokens, lax.axis_index("tensor") * half_width, half_width, 1
    )
    outgoing = jnp.zeros((experts_all * capacity, half_width), jnp.bfloat16)
    outgoing = outgoing.at[slot_index].set(jnp.repeat(own_cols, top_count, axis=0))
    outgoing = outgoing.reshape(experts_all, capacity, half_width)
    received = lax.all_to_all(outgoing, "expert", split_axis=0, concat_axis=0, tiled=True)
    received = lax.all_gather(received, "tensor", axis=2, tiled=True)
    item_rows = received.shape[1]
    stacked = received.reshape(expert_count, local_experts, item_rows, width_all)
    stacked = stacked.transpose(1, 0, 2, 3).reshape(
        local_experts, expert_count * item_rows, width_all
    )
    gate_val = jnp.einsum("emd,edf->emf", stacked, w_gate, preferred_element_type=jnp.float32)
    up_val = jnp.einsum("emd,edf->emf", stacked, w_up, preferred_element_type=jnp.float32)
    hidden = (jax.nn.silu(gate_val) * up_val).astype(jnp.bfloat16)
    partial_value = jnp.einsum("emf,efd->emd", hidden, w_down, preferred_element_type=jnp.float32)
    partial_value = partial_value.reshape(local_experts, expert_count, item_rows, width_all)
    partial_value = partial_value.transpose(1, 0, 2, 3).reshape(experts_all, item_rows, width_all)
    summed = lax.psum_scatter(partial_value, "tensor", scatter_dimension=2, tiled=True).astype(
        jnp.bfloat16
    )
    returned = lax.all_to_all(summed, "expert", split_axis=0, concat_axis=0, tiled=True)
    shared_g = jnp.dot(tokens, shared_gate, preferred_element_type=jnp.float32)
    shared_u = jnp.dot(tokens, shared_up, preferred_element_type=jnp.float32)
    shared_hidden = (jax.nn.silu(shared_g) * shared_u).astype(jnp.bfloat16)
    shared_part = jnp.dot(shared_hidden, shared_down, preferred_element_type=jnp.float32)
    picked = returned.reshape(experts_all * capacity, half_width)[slot_index]
    picked = picked.astype(jnp.float32).reshape(tok_count, top_count, half_width)
    routed = jnp.sum(gates[:, :, None] * picked, axis=1)
    total = routed + lax.psum_scatter(shared_part, "tensor", scatter_dimension=1, tiled=True)
    return (own_cols.astype(jnp.float32) + total).astype(jnp.bfloat16)


def silu_mul(g, u):
    return (g / (1.0 + jnp.exp(-g)) * u).astype(jnp.bfloat16)


def moe_kernel(nz, nx, width, ext_ref, tok_ref, wg_ref, wu_ref, wd_ref, sg_ref, su_ref, sd_ref, out_ref,
               X, Wg, Wu, Wd, Sg, Su, Sd, OWN, O, PXs, PXr, CSs, CSr, SHo, SHs, SHr, FXs, FXr,
               w_loc, s_loc, w_send, w_recv, z_send, z_recv, x_send, x_recv, p_send, p_recv,
               c_send, c_recv, m_send, m_recv):
    me = lax.axis_index("expert")
    core = lax.axis_index("tensor")
    z = me // nx
    x = me % nx
    ox = nx - 1 - x
    other = z * nx + ox
    rows = ext_ref.shape[0]
    half = out_ref.shape[1]

    barrier = pltpu.get_barrier_semaphore()
    for d in range(1, nz):
        peer = ((z + d) % nz) * nx + x
        pl.semaphore_signal(barrier, inc=1, device_id={"expert": peer}, device_id_type=MESH)
    pl.semaphore_signal(barrier, inc=1, device_id={"expert": other}, device_id_type=MESH)
    pl.semaphore_signal(barrier, inc=1, device_id={"tensor": 1 - core}, device_id_type=MESH)

    loc_s = [pltpu.make_async_copy(a, b, s_loc.at[i]) for i, (a, b) in enumerate(
        ((sg_ref, Sg), (su_ref, Su), (sd_ref, Sd)))]
    loc_w = [pltpu.make_async_copy(a.at[0], b.at[0], w_loc.at[i]) for i, (a, b) in enumerate(
        ((wg_ref, Wg), (wu_ref, Wu), (wd_ref, Wd)))]
    for cp in loc_s + loc_w:
        cp.start()
    X[me] = ext_ref[...]
    pl.semaphore_wait(barrier, nz + 1)

    def remote(src, dst, ssem, rsem, **dev):
        return pltpu.make_async_remote_copy(src_ref=src, dst_ref=dst, send_sem=ssem, recv_sem=rsem,
                                            device_id=dev, device_id_type=MESH)

    def z_copy(zo, side):
        e = zo * nx + x
        peer = me + nx if side == 0 else me - nx
        return remote(X.at[e], X.at[e], z_send.at[side, zo], z_recv.at[zo], expert=peer)

    def x_copy(zo, col):
        e = zo * nx + col
        return remote(X.at[e], X.at[e], x_send.at[zo], x_recv.at[zo], expert=other)

    def forward(zo):
        @pl.when(jnp.logical_and(zo <= z, z + 1 < nz))
        def _():
            z_copy(zo, 0).start()

        @pl.when(jnp.logical_and(zo >= z, z >= 1))
        def _():
            z_copy(zo, 1).start()

        x_copy(zo, x).start()

    def p_copy(zo):
        return remote(PXs.at[zo], PXr.at[zo], p_send.at[zo], p_recv.at[zo], expert=other)

    def c_copy(zo, slot):
        return remote(CSs.at[zo], CSr.at[slot], c_send.at[zo], c_recv.at[slot], expert=zo * nx + x)

    forward(z)
    rem_w = [remote(a.at[0], b.at[1], w_send.at[i], w_recv.at[i], tensor=1 - core) for i, (a, b) in enumerate(
        ((wg_ref, Wg), (wu_ref, Wu), (wd_ref, Wd)))]
    for cp in rem_w:
        cp.start()

    table = [sorted(range(nz), key=lambda q: (abs(q - k), q)) for k in range(nz)]

    def nth(i):
        r = table[0][i]
        for k in range(1, nz):
            r = jnp.where(z == k, table[k][i], r)
        return r

    for cp in loc_s:
        cp.wait()
    tok = tok_ref[...]
    sh = silu_mul(jnp.dot(tok, Sg[...], preferred_element_type=jnp.float32),
                  jnp.dot(tok, Su[...], preferred_element_type=jnp.float32))
    SHo[...] = jnp.dot(sh, Sd[...], preferred_element_type=jnp.float32)

    @pl.when(core == 0)
    def _():
        SHs[...] = SHo[:, half:]

    @pl.when(core == 1)
    def _():
        SHs[...] = SHo[:, :half]
    sh_copy = remote(SHs, SHr, m_send.at[0], m_recv.at[0], tensor=1 - core)
    sh_copy.start()

    for cp in loc_w:
        cp.wait()
    for cp in rem_w:
        cp.wait_recv()

    def compute(zo):
        base = zo * nx
        xs = X[pl.ds(base, nx)].reshape(nx * rows, X.shape[2])
        xin = xs[:, :width]
        O[...] = jnp.zeros_like(O)
        for hh in range(2):
            hid = silu_mul(jnp.dot(xin, Wg[hh], preferred_element_type=jnp.float32),
                           jnp.dot(xin, Wu[hh], preferred_element_type=jnp.float32))
            O[...] += jnp.dot(hid, Wd[hh], preferred_element_type=jnp.float32)
        lo = width // 128 * 128
        tail = xs[:, lo:].astype(jnp.float32)
        lane = lax.broadcasted_iota(jnp.int32, tail.shape, 1) - (width - lo)
        n_all = nz * nx
        hit = (lane == me) | (lane == me + n_all) | (lane == me + 2 * n_all)
        weight = jnp.sum(jnp.where(hit, tail, 0.0), axis=1, keepdims=True)
        O[...] = weight * O[...].astype(jnp.bfloat16).astype(jnp.float32)
        OWN[zo] = O[pl.ds(pl.multiple_of(x * rows, rows), rows), :]
        PXs[zo] = O[pl.ds(pl.multiple_of(ox * rows, rows), rows), :].astype(jnp.bfloat16)

    def column_sum(zo):
        p_copy(zo).wait_recv()
        CSs[zo] = (OWN[zo] + PXr[zo].astype(jnp.float32)).astype(jnp.bfloat16)
        c_copy(zo, z).start()

    for i in range(nz):
        zi = nth(i)
        if i + 1 < nz:
            zn = nth(i + 1)
            z_copy(zn, 0).wait_recv()
            forward(zn)
        if i >= 3:
            column_sum(nth(i - 2))
        x_copy(zi, ox).wait_recv()
        compute(zi)
        if i > 0:
            p_copy(zi).start()
    p_copy(z).start()
    for i in range(max(1, nz - 2), nz):
        column_sum(nth(i))
    p_copy(z).wait_recv()
    OWN[z] += PXr[z].astype(jnp.float32)
    for i in range(1, nz):
        zi = nth(i)
        c_copy(zi, zi).wait_recv()
        OWN[z] += CSr[zi].astype(jnp.float32)

    @pl.when(core == 0)
    def _():
        FXs[...] = OWN[z, :, half:]

    @pl.when(core == 1)
    def _():
        FXs[...] = OWN[z, :, :half]
    fx_copy = remote(FXs, FXr, m_send.at[1], m_recv.at[1], tensor=1 - core)
    fx_copy.start()
    sh_copy.wait_recv()
    fx_copy.wait_recv()

    for cc in range(2):
        @pl.when(core == cc)
        def _():
            cols = slice(cc * half, (cc + 1) * half)
            for hh in range(2):
                rr = slice(hh * rows, (hh + 1) * rows)
                routed = OWN[z, :, cols] if hh == cc else FXr[...]
                total = tok_ref[rr, cols].astype(jnp.float32) + routed + (SHo[rr, cols] + SHr[rr, :])
                out_ref[rr, :] = total.astype(jnp.bfloat16)

    for cp in rem_w:
        cp.wait_send()
    sh_copy.wait_send()
    fx_copy.wait_send()
    for i in range(nz):
        zo = i

        @pl.when(jnp.logical_and(zo <= z, z + 1 < nz))
        def _():
            z_copy(zo, 0).wait_send()

        @pl.when(jnp.logical_and(zo >= z, z >= 1))
        def _():
            z_copy(zo, 1).wait_send()

        x_copy(zo, x).wait_send()
        p_copy(zo).wait_send()

        @pl.when(zo != z)
        def _():
            c_copy(zo, z).wait_send()


def pad(n, m):
    return -(-n // m) * m


def gather_plan(tok_count, width, expert_count, local_experts, hidden):
    if local_experts != 1 or expert_count % 2 or tok_count % 32 or width % 2:
        return None
    nz, rows = expert_count // 2, tok_count // 2
    ext = pad(width + 3 * expert_count, 128)
    if ext - width // 128 * 128 > 128:
        return None
    wide, hid, half = pad(width, 128), pad(hidden, 128), pad(width // 2, 128)
    weights = 9 * (2 * width * hid + pad(hidden, 16) * wide) * 2 // 3 + 0
    moved = expert_count * rows * ext * 2 + 4 * nz * rows * wide * 2 + nz * rows * wide * 4
    flat = tok_count * (2 * wide * 4 + 2 * half * 4 + 2 * wide * 2) + 2 * rows * half * 4
    return weights + moved + flat


def gather_local(tokens, routes, gates, w_gate, w_up, w_down, shared_gate, shared_up, shared_down):
    tok_count, width = tokens.shape
    hidden = w_gate.shape[2]
    n = lax.axis_size("expert")
    nx, nz = 2, n // 2
    rows, half = tok_count // 2, width // 2
    ext_w = pad(width + 3 * n, 128)
    core = lax.axis_index("tensor")
    first = core * rows
    toks = lax.dynamic_slice_in_dim(tokens, first, rows, 0)
    rts = lax.dynamic_slice_in_dim(routes, first, rows, 0)
    gts = lax.dynamic_slice_in_dim(gates, first, rows, 0)
    named = rts[:, :, None] == jnp.arange(n, dtype=jnp.int32)[None, None, :]
    dense = jnp.sum(jnp.where(named, gts[:, :, None], 0.0), axis=1)
    hi = lax.reduce_precision(dense, 8, 7)
    mid = lax.reduce_precision(dense - hi, 8, 7)
    low = dense - hi - mid
    terms = jnp.concatenate([hi, mid, low, jnp.zeros((rows, ext_w - width - 3 * n), jnp.float32)], 1)
    ext = jnp.concatenate([toks, terms.astype(jnp.bfloat16)], 1)
    bf, f32 = jnp.bfloat16, jnp.float32
    vm, dma = pltpu.VMEM, pltpu.SemaphoreType.DMA
    scratch = [
        vm((n, rows, ext_w), bf),
        vm((2, width, hidden), bf), vm((2, width, hidden), bf), vm((2, hidden, width), bf),
        vm((width, hidden), bf), vm((width, hidden), bf), vm((hidden, width), bf),
        vm((nz, rows, width), f32), vm((nx * rows, width), f32),
        vm((nz, rows, width), bf), vm((nz, rows, width), bf), vm((nz, rows, width), bf), vm((nz, rows, width), bf),
        vm((tok_count, width), f32), vm((tok_count, half), f32), vm((tok_count, half), f32),
        vm((rows, half), f32), vm((rows, half), f32),
        dma((3,)), dma((3,)), dma((3,)), dma((3,)), dma((2, nz)), dma((nz,)), dma((nz,)), dma((nz,)),
        dma((nz,)), dma((nz,)), dma((nz,)), dma((nz,)), dma((2,)), dma((2,)),
    ]
    in_vmem, in_hbm = pl.BlockSpec(memory_space=pltpu.VMEM), pl.BlockSpec(memory_space=pl.ANY)
    return pl.pallas_call(
        functools.partial(moe_kernel, nz, nx, width),
        out_shape=jax.ShapeDtypeStruct((tok_count, half), bf),
        in_specs=[in_vmem] * 2 + [in_hbm] * 6,
        out_specs=in_vmem,
        scratch_shapes=scratch,
        compiler_params=pltpu.CompilerParams(collective_id=0, has_side_effects=True, vmem_limit_bytes=60 * 1024 * 1024),
    )(ext, tokens, w_gate, w_up, w_down, shared_gate, shared_up, shared_down)


def local(tokens, routes, gates, w_gate, *rest):
    need = gather_plan(*tokens.shape, lax.axis_size("expert"), w_gate.shape[0], w_gate.shape[2])
    if need is not None and lax.axis_size("tensor") == 2 and need <= VMEM_BUDGET:
        return gather_local(tokens, routes, gates, w_gate, *rest)
    return exchange_local(tokens, routes, gates, w_gate, *rest)


def solution(mesh):
    in_specs = (
        P(("groups", "expert"), None),
        P(("groups", "expert"), None),
        P(("groups", "expert"), None),
        P("expert", None, "tensor"),
        P("expert", None, "tensor"),
        P("expert", "tensor", None),
        P(None, "tensor"),
        P(None, "tensor"),
        P("tensor", None),
    )
    out_specs = P(("groups", "expert"), "tensor")
    return jax.shard_map(local, mesh=mesh, in_specs=in_specs, out_specs=out_specs, check_vma=False)
```

```python
import functools

import jax
import jax.numpy as jnp
from jax import lax
from jax.experimental import pallas as pl
from jax.experimental.pallas import tpu as pltpu
from jax.sharding import PartitionSpec as P

MESH = pl.DeviceIdType.MESH
VMEM_BUDGET = 52 * 1024 * 1024


def exchange_local(tokens, routes, gates, w_gate, w_up, w_down, shared_gate, shared_up, shared_down):
    tok_count, top_count = routes.shape
    width_all = tokens.shape[1]
    local_experts = w_gate.shape[0]
    expert_count = lax.axis_size("expert")
    experts_all = expert_count * local_experts
    capacity = max(2, (3 * tok_count * top_count + 2 * experts_all - 1) // (2 * experts_all))
    flat_routes = routes.reshape(-1)
    onehot = (flat_routes[:, None] == jnp.arange(experts_all, dtype=jnp.int32)[None, :]).astype(
        jnp.int32
    )
    order_in = jnp.sum(jnp.cumsum(onehot, axis=0) * onehot, axis=1) - 1
    slot_index = flat_routes * capacity + order_in
    half_width = width_all // lax.axis_size("tensor")
    own_cols = lax.dynamic_slice_in_dim(
        tokens, lax.axis_index("tensor") * half_width, half_width, 1
    )
    outgoing = jnp.zeros((experts_all * capacity, half_width), jnp.bfloat16)
    outgoing = outgoing.at[slot_index].set(jnp.repeat(own_cols, top_count, axis=0))
    outgoing = outgoing.reshape(experts_all, capacity, half_width)
    received = lax.all_to_all(outgoing, "expert", split_axis=0, concat_axis=0, tiled=True)
    received = lax.all_gather(received, "tensor", axis=2, tiled=True)
    item_rows = received.shape[1]
    stacked = received.reshape(expert_count, local_experts, item_rows, width_all)
    stacked = stacked.transpose(1, 0, 2, 3).reshape(
        local_experts, expert_count * item_rows, width_all
    )
    gate_val = jnp.einsum("emd,edf->emf", stacked, w_gate, preferred_element_type=jnp.float32)
    up_val = jnp.einsum("emd,edf->emf", stacked, w_up, preferred_element_type=jnp.float32)
    hidden = (jax.nn.silu(gate_val) * up_val).astype(jnp.bfloat16)
    partial_value = jnp.einsum("emf,efd->emd", hidden, w_down, preferred_element_type=jnp.float32)
    partial_value = partial_value.reshape(local_experts, expert_count, item_rows, width_all)
    partial_value = partial_value.transpose(1, 0, 2, 3).reshape(experts_all, item_rows, width_all)
    summed = lax.psum_scatter(partial_value, "tensor", scatter_dimension=2, tiled=True).astype(
        jnp.bfloat16
    )
    returned = lax.all_to_all(summed, "expert", split_axis=0, concat_axis=0, tiled=True)
    shared_g = jnp.dot(tokens, shared_gate, preferred_element_type=jnp.float32)
    shared_u = jnp.dot(tokens, shared_up, preferred_element_type=jnp.float32)
    shared_hidden = (jax.nn.silu(shared_g) * shared_u).astype(jnp.bfloat16)
    shared_part = jnp.dot(shared_hidden, shared_down, preferred_element_type=jnp.float32)
    picked = returned.reshape(experts_all * capacity, half_width)[slot_index]
    picked = picked.astype(jnp.float32).reshape(tok_count, top_count, half_width)
    routed = jnp.sum(gates[:, :, None] * picked, axis=1)
    total = routed + lax.psum_scatter(shared_part, "tensor", scatter_dimension=1, tiled=True)
    return (own_cols.astype(jnp.float32) + total).astype(jnp.bfloat16)


def silu_mul(g, u):
    return (g / (1.0 + jnp.exp(-g)) * u).astype(jnp.bfloat16)


def moe_kernel(nz, nx, width, tok_ref, routes_ref, gates_ref, wg_ref, wu_ref, wd_ref, sg_ref, su_ref, sd_ref, out_ref,
               X, Wg, Wu, Wd, Sg, Su, Sd, OWN, O, PXs, PXr, CSs, CSr, SHo, SHs, SHr, FXs, FXr,
               w_loc, s_loc, w_send, w_recv, z_send, z_recv, x_send, x_recv, p_send, p_recv,
               c_send, c_recv, m_send, m_recv):
    me = lax.axis_index("expert")
    core = lax.axis_index("tensor")
    z = me // nx
    x = me % nx
    ox = nx - 1 - x
    other = z * nx + ox
    rows = tok_ref.shape[0] // 2
    half = out_ref.shape[1]

    barrier = pltpu.get_barrier_semaphore()
    for d in range(1, nz):
        peer = ((z + d) % nz) * nx + x
        pl.semaphore_signal(barrier, inc=1, device_id={"expert": peer}, device_id_type=MESH)
    pl.semaphore_signal(barrier, inc=1, device_id={"expert": other}, device_id_type=MESH)
    pl.semaphore_signal(barrier, inc=1, device_id={"tensor": 1 - core}, device_id_type=MESH)

    loc_s = [pltpu.make_async_copy(a, b, s_loc.at[i]) for i, (a, b) in enumerate(
        ((sg_ref, Sg), (su_ref, Su), (sd_ref, Sd)))]
    loc_w = [pltpu.make_async_copy(a.at[0], b.at[0], w_loc.at[i]) for i, (a, b) in enumerate(
        ((wg_ref, Wg), (wu_ref, Wu), (wd_ref, Wd)))]
    for cp in loc_s + loc_w:
        cp.start()
    n_all = nz * nx
    lo = width // 128 * 128
    spare = X.shape[2] - lo

    def own_half(ref):
        return jnp.where(core == 0, ref[:, :rows], ref[:, rows:])
    named, gate = own_half(routes_ref), own_half(gates_ref)
    slot = lax.broadcasted_iota(jnp.int32, (spare, rows), 0) - (width - lo)
    dense = jnp.zeros((spare, rows), jnp.float32)
    for k in range(named.shape[0]):
        for term in range(3):
            dense = jnp.where(slot - term * n_all == named[k:k + 1, :], gate[k:k + 1, :], dense)
    hi = dense.astype(jnp.bfloat16).astype(jnp.float32)
    mid = (dense - hi).astype(jnp.bfloat16).astype(jnp.float32)
    low = dense - hi - mid
    terms = jnp.where(slot < n_all, hi, jnp.where(slot < 2 * n_all, mid, low))
    X[me, :, lo:] = terms.T.astype(jnp.bfloat16)
    X[me, :, :width] = tok_ref[pl.ds(pl.multiple_of(core * rows, rows), rows), :]
    pl.semaphore_wait(barrier, nz + 1)

    def remote(src, dst, ssem, rsem, **dev):
        return pltpu.make_async_remote_copy(src_ref=src, dst_ref=dst, send_sem=ssem, recv_sem=rsem,
                                            device_id=dev, device_id_type=MESH)

    def z_copy(zo, side):
        e = zo * nx + x
        peer = me + nx if side == 0 else me - nx
        return remote(X.at[e], X.at[e], z_send.at[side, zo], z_recv.at[zo], expert=peer)

    def x_copy(zo, col):
        e = zo * nx + col
        return remote(X.at[e], X.at[e], x_send.at[zo], x_recv.at[zo], expert=other)

    def forward_z(zo):
        @pl.when(jnp.logical_and(zo <= z, z + 1 < nz))
        def _():
            z_copy(zo, 0).start()

        @pl.when(jnp.logical_and(zo >= z, z >= 1))
        def _():
            z_copy(zo, 1).start()

    def forward_x(zo):
        x_copy(zo, x).start()

    def take_z(zo):
        z_copy(zo, 0).wait_recv()
        forward_z(zo)

    def p_copy(zo):
        return remote(PXs.at[zo], PXr.at[zo], p_send.at[zo], p_recv.at[zo], expert=other)

    def c_copy(zo, slot):
        return remote(CSs.at[zo], CSr.at[slot], c_send.at[zo], c_recv.at[slot], expert=zo * nx + x)

    forward_z(z)
    forward_x(z)
    rem_w = [remote(a.at[0], b.at[1], w_send.at[i], w_recv.at[i], tensor=1 - core) for i, (a, b) in enumerate(
        ((wg_ref, Wg), (wu_ref, Wu), (wd_ref, Wd)))]
    for cp in rem_w:
        cp.start()

    table = [sorted(range(nz), key=lambda q: (abs(q - k), abs(2 * q + 1 - nz))) for k in range(nz)]

    def nth(i):
        r = table[0][i]
        for k in range(1, nz):
            r = jnp.where(z == k, table[k][i], r)
        return r

    for cp in loc_s:
        cp.wait()
    tok = tok_ref[...]
    sh = silu_mul(jnp.dot(tok, Sg[...], preferred_element_type=jnp.float32),
                  jnp.dot(tok, Su[...], preferred_element_type=jnp.float32))
    SHo[...] = jnp.dot(sh, Sd[...], preferred_element_type=jnp.float32)

    @pl.when(core == 0)
    def _():
        SHs[...] = SHo[:, half:]

    @pl.when(core == 1)
    def _():
        SHs[...] = SHo[:, :half]
    sh_copy = remote(SHs, SHr, m_send.at[0], m_recv.at[0], tensor=1 - core)
    sh_copy.start()

    for cp in loc_w:
        cp.wait()
    for cp in rem_w:
        cp.wait_recv()

    def compute(zo):
        base = zo * nx
        xs = X[pl.ds(base, nx)].reshape(nx * rows, X.shape[2])
        xin = xs[:, :width]
        O[...] = jnp.zeros_like(O)
        for hh in range(2):
            hid = silu_mul(jnp.dot(xin, Wg[hh], preferred_element_type=jnp.float32),
                           jnp.dot(xin, Wu[hh], preferred_element_type=jnp.float32))
            O[...] += jnp.dot(hid, Wd[hh], preferred_element_type=jnp.float32)
        tail = xs[:, lo:].astype(jnp.float32)
        lane = lax.broadcasted_iota(jnp.int32, tail.shape, 1) - (width - lo)
        hit = (lane == me) | (lane == me + n_all) | (lane == me + 2 * n_all)
        weight = jnp.sum(jnp.where(hit, tail, 0.0), axis=1, keepdims=True)
        O[...] = weight * O[...].astype(jnp.bfloat16).astype(jnp.float32)
        OWN[zo] = O[pl.ds(pl.multiple_of(x * rows, rows), rows), :]
        PXs[zo] = O[pl.ds(pl.multiple_of(ox * rows, rows), rows), :].astype(jnp.bfloat16)

    def column_sum(zo):
        p_copy(zo).wait_recv()
        CSs[zo] = (OWN[zo] + PXr[zo].astype(jnp.float32)).astype(jnp.bfloat16)
        c_copy(zo, z).start()

    for i in range(nz):
        zi = nth(i)

        @pl.when(jnp.logical_or(z == 0, z == nz - 1))
        def _():
            if i + 1 < nz:
                take_z(nth(i + 1))
                forward_x(nth(i + 1))

        @pl.when(jnp.logical_and(z > 0, z < nz - 1))
        def _():
            if i == 0:
                for j in range(1, min(3, nz)):
                    take_z(nth(j))
                    forward_x(nth(j))
            else:
                if i + 2 < nz:
                    take_z(nth(i + 2))
                if 2 <= i < nz - 1:
                    forward_x(nth(i + 1))
        if i >= 3:
            column_sum(nth(i - 2))
        x_copy(zi, ox).wait_recv()
        compute(zi)
        if i > 0:
            p_copy(zi).start()
    p_copy(z).start()
    for i in range(max(1, nz - 2), nz):
        column_sum(nth(i))
    p_copy(z).wait_recv()
    OWN[z] += PXr[z].astype(jnp.float32)
    for i in range(1, nz):
        zi = nth(i)
        c_copy(zi, zi).wait_recv()
        OWN[z] += CSr[zi].astype(jnp.float32)

    @pl.when(core == 0)
    def _():
        FXs[...] = OWN[z, :, half:]

    @pl.when(core == 1)
    def _():
        FXs[...] = OWN[z, :, :half]
    fx_copy = remote(FXs, FXr, m_send.at[1], m_recv.at[1], tensor=1 - core)
    fx_copy.start()
    sh_copy.wait_recv()
    fx_copy.wait_recv()

    for cc in range(2):
        @pl.when(core == cc)
        def _():
            cols = slice(cc * half, (cc + 1) * half)
            for hh in range(2):
                rr = slice(hh * rows, (hh + 1) * rows)
                routed = OWN[z, :, cols] if hh == cc else FXr[...]
                total = tok_ref[rr, cols].astype(jnp.float32) + routed + (SHo[rr, cols] + SHr[rr, :])
                out_ref[rr, :] = total.astype(jnp.bfloat16)

    for cp in rem_w:
        cp.wait_send()
    sh_copy.wait_send()
    fx_copy.wait_send()
    for i in range(nz):
        zo = i

        @pl.when(jnp.logical_and(zo <= z, z + 1 < nz))
        def _():
            z_copy(zo, 0).wait_send()

        @pl.when(jnp.logical_and(zo >= z, z >= 1))
        def _():
            z_copy(zo, 1).wait_send()

        x_copy(zo, x).wait_send()
        p_copy(zo).wait_send()

        @pl.when(zo != z)
        def _():
            c_copy(zo, z).wait_send()


def pad(n, m):
    return -(-n // m) * m


def gather_plan(tok_count, width, expert_count, local_experts, hidden):
    if local_experts != 1 or expert_count % 2 or tok_count % 32 or width % 2:
        return None
    nz, rows = expert_count // 2, tok_count // 2
    ext = pad(width + 3 * expert_count, 128)
    if ext - width // 128 * 128 > 128:
        return None
    wide, hid, half = pad(width, 128), pad(hidden, 128), pad(width // 2, 128)
    weights = 9 * (2 * width * hid + pad(hidden, 16) * wide) * 2 // 3 + 0
    moved = expert_count * rows * ext * 2 + 4 * nz * rows * wide * 2 + nz * rows * wide * 4
    flat = tok_count * (2 * wide * 4 + 2 * half * 4 + 2 * wide * 2) + 2 * rows * half * 4
    return weights + moved + flat


def gather_local(tokens, routes, gates, w_gate, w_up, w_down, shared_gate, shared_up, shared_down):
    tok_count, width = tokens.shape
    hidden = w_gate.shape[2]
    n = lax.axis_size("expert")
    nx, nz = 2, n // 2
    rows, half = tok_count // 2, width // 2
    ext_w = pad(width + 3 * n, 128)
    bf, f32 = jnp.bfloat16, jnp.float32
    vm, dma = pltpu.VMEM, pltpu.SemaphoreType.DMA
    scratch = [
        vm((n, rows, ext_w), bf),
        vm((2, width, hidden), bf), vm((2, width, hidden), bf), vm((2, hidden, width), bf),
        vm((width, hidden), bf), vm((width, hidden), bf), vm((hidden, width), bf),
        vm((nz, rows, width), f32), vm((nx * rows, width), f32),
        vm((nz, rows, width), bf), vm((nz, rows, width), bf), vm((nz, rows, width), bf), vm((nz, rows, width), bf),
        vm((tok_count, width), f32), vm((tok_count, half), f32), vm((tok_count, half), f32),
        vm((rows, half), f32), vm((rows, half), f32),
        dma((3,)), dma((3,)), dma((3,)), dma((3,)), dma((2, nz)), dma((nz,)), dma((nz,)), dma((nz,)),
        dma((nz,)), dma((nz,)), dma((nz,)), dma((nz,)), dma((2,)), dma((2,)),
    ]
    in_vmem, in_hbm = pl.BlockSpec(memory_space=pltpu.VMEM), pl.BlockSpec(memory_space=pl.ANY)
    return pl.pallas_call(
        functools.partial(moe_kernel, nz, nx, width),
        out_shape=jax.ShapeDtypeStruct((tok_count, half), bf),
        in_specs=[in_vmem] * 3 + [in_hbm] * 6,
        out_specs=in_vmem,
        scratch_shapes=scratch,
        compiler_params=pltpu.CompilerParams(collective_id=0, has_side_effects=True, vmem_limit_bytes=60 * 1024 * 1024),
    )(tokens, routes.T, gates.T, w_gate, w_up, w_down, shared_gate, shared_up, shared_down)


def local(tokens, routes, gates, w_gate, *rest):
    need = gather_plan(*tokens.shape, lax.axis_size("expert"), w_gate.shape[0], w_gate.shape[2])
    if need is not None and lax.axis_size("tensor") == 2 and need <= VMEM_BUDGET:
        return gather_local(tokens, routes, gates, w_gate, *rest)
    return exchange_local(tokens, routes, gates, w_gate, *rest)


def solution(mesh):
    in_specs = (
        P(("groups", "expert"), None),
        P(("groups", "expert"), None),
        P(("groups", "expert"), None),
        P("expert", None, "tensor"),
        P("expert", None, "tensor"),
        P("expert", "tensor", None),
        P(None, "tensor"),
        P(None, "tensor"),
        P("tensor", None),
    )
    out_specs = P(("groups", "expert"), "tensor")
    return jax.shard_map(local, mesh=mesh, in_specs=in_specs, out_specs=out_specs, check_vma=False)
```

```python
import functools

import jax
import jax.numpy as jnp
from jax import lax
from jax.experimental import pallas as pl
from jax.experimental.pallas import tpu as pltpu
from jax.sharding import PartitionSpec as P

MESH = pl.DeviceIdType.MESH
VMEM_BUDGET = 52 * 1024 * 1024


def exchange_local(tokens, routes, gates, w_gate, w_up, w_down, shared_gate, shared_up, shared_down):
    tok_count, top_count = routes.shape
    width_all = tokens.shape[1]
    local_experts = w_gate.shape[0]
    expert_count = lax.axis_size("expert")
    experts_all = expert_count * local_experts
    capacity = max(2, (3 * tok_count * top_count + 2 * experts_all - 1) // (2 * experts_all))
    flat_routes = routes.reshape(-1)
    onehot = (flat_routes[:, None] == jnp.arange(experts_all, dtype=jnp.int32)[None, :]).astype(
        jnp.int32
    )
    order_in = jnp.sum(jnp.cumsum(onehot, axis=0) * onehot, axis=1) - 1
    slot_index = flat_routes * capacity + order_in
    half_width = width_all // lax.axis_size("tensor")
    own_cols = lax.dynamic_slice_in_dim(
        tokens, lax.axis_index("tensor") * half_width, half_width, 1
    )
    outgoing = jnp.zeros((experts_all * capacity, half_width), jnp.bfloat16)
    outgoing = outgoing.at[slot_index].set(jnp.repeat(own_cols, top_count, axis=0))
    outgoing = outgoing.reshape(experts_all, capacity, half_width)
    received = lax.all_to_all(outgoing, "expert", split_axis=0, concat_axis=0, tiled=True)
    received = lax.all_gather(received, "tensor", axis=2, tiled=True)
    item_rows = received.shape[1]
    stacked = received.reshape(expert_count, local_experts, item_rows, width_all)
    stacked = stacked.transpose(1, 0, 2, 3).reshape(
        local_experts, expert_count * item_rows, width_all
    )
    gate_val = jnp.einsum("emd,edf->emf", stacked, w_gate, preferred_element_type=jnp.float32)
    up_val = jnp.einsum("emd,edf->emf", stacked, w_up, preferred_element_type=jnp.float32)
    hidden = (jax.nn.silu(gate_val) * up_val).astype(jnp.bfloat16)
    partial_value = jnp.einsum("emf,efd->emd", hidden, w_down, preferred_element_type=jnp.float32)
    partial_value = partial_value.reshape(local_experts, expert_count, item_rows, width_all)
    partial_value = partial_value.transpose(1, 0, 2, 3).reshape(experts_all, item_rows, width_all)
    summed = lax.psum_scatter(partial_value, "tensor", scatter_dimension=2, tiled=True).astype(
        jnp.bfloat16
    )
    returned = lax.all_to_all(summed, "expert", split_axis=0, concat_axis=0, tiled=True)
    shared_g = jnp.dot(tokens, shared_gate, preferred_element_type=jnp.float32)
    shared_u = jnp.dot(tokens, shared_up, preferred_element_type=jnp.float32)
    shared_hidden = (jax.nn.silu(shared_g) * shared_u).astype(jnp.bfloat16)
    shared_part = jnp.dot(shared_hidden, shared_down, preferred_element_type=jnp.float32)
    picked = returned.reshape(experts_all * capacity, half_width)[slot_index]
    picked = picked.astype(jnp.float32).reshape(tok_count, top_count, half_width)
    routed = jnp.sum(gates[:, :, None] * picked, axis=1)
    total = routed + lax.psum_scatter(shared_part, "tensor", scatter_dimension=1, tiled=True)
    return (own_cols.astype(jnp.float32) + total).astype(jnp.bfloat16)


def silu_mul(g, u):
    return (g / (1.0 + jnp.exp(-g)) * u).astype(jnp.bfloat16)


def moe_kernel(nz, nx, width, tok_ref, routes_ref, gates_ref, wg_ref, wu_ref, wd_ref, sg_ref, su_ref, sd_ref, out_ref,
               X, Wg, Wu, Wd, Sg, Su, Sd, OWN, O, PXs, PXr, CSs, CSr, SHo, SHs, SHr, FXs, FXr,
               w_loc, s_loc, w_send, w_recv, z_send, z_recv, x_send, x_recv, p_send, p_recv,
               c_send, c_recv, m_send, m_recv):
    me = lax.axis_index("expert")
    core = lax.axis_index("tensor")
    z = me // nx
    x = me % nx
    ox = nx - 1 - x
    other = z * nx + ox
    rows = tok_ref.shape[0] // 2
    half = out_ref.shape[1]

    barrier = pltpu.get_barrier_semaphore()
    for d in range(1, nz):
        peer = ((z + d) % nz) * nx + x
        pl.semaphore_signal(barrier, inc=1, device_id={"expert": peer}, device_id_type=MESH)
    pl.semaphore_signal(barrier, inc=1, device_id={"expert": other}, device_id_type=MESH)
    pl.semaphore_signal(barrier, inc=1, device_id={"tensor": 1 - core}, device_id_type=MESH)

    loc_s = [pltpu.make_async_copy(a, b, s_loc.at[i]) for i, (a, b) in enumerate(
        ((sg_ref, Sg), (su_ref, Su), (sd_ref, Sd)))]
    loc_w = [pltpu.make_async_copy(a.at[0], b.at[0], w_loc.at[i]) for i, (a, b) in enumerate(
        ((wg_ref, Wg), (wu_ref, Wu), (wd_ref, Wd)))]
    for cp in loc_s + loc_w:
        cp.start()
    n_all = nz * nx
    lo = width // 128 * 128
    spare = X.shape[2] - lo

    def own_half(ref):
        return jnp.where(core == 0, ref[:, :rows], ref[:, rows:])
    named, gate = own_half(routes_ref), own_half(gates_ref)
    slot = lax.broadcasted_iota(jnp.int32, (spare, rows), 0) - (width - lo)
    dense = jnp.zeros((spare, rows), jnp.float32)
    for k in range(named.shape[0]):
        for term in range(3):
            dense = jnp.where(slot - term * n_all == named[k:k + 1, :], gate[k:k + 1, :], dense)
    hi = dense.astype(jnp.bfloat16).astype(jnp.float32)
    mid = (dense - hi).astype(jnp.bfloat16).astype(jnp.float32)
    low = dense - hi - mid
    terms = jnp.where(slot < n_all, hi, jnp.where(slot < 2 * n_all, mid, low))
    X[me, :, lo:] = terms.T.astype(jnp.bfloat16)
    X[me, :, :width] = tok_ref[pl.ds(pl.multiple_of(core * rows, rows), rows), :]
    pl.semaphore_wait(barrier, nz + 1)

    def remote(src, dst, ssem, rsem, **dev):
        return pltpu.make_async_remote_copy(src_ref=src, dst_ref=dst, send_sem=ssem, recv_sem=rsem,
                                            device_id=dev, device_id_type=MESH)

    def z_copy(zo, side):
        e = zo * nx + x
        peer = me + nx if side == 0 else me - nx
        return remote(X.at[e], X.at[e], z_send.at[side, zo], z_recv.at[zo], expert=peer)

    def x_copy(zo, col):
        e = zo * nx + col
        return remote(X.at[e], X.at[e], x_send.at[zo], x_recv.at[zo], expert=other)

    def forward_z(zo):
        @pl.when(jnp.logical_and(zo <= z, z + 1 < nz))
        def _():
            z_copy(zo, 0).start()

        @pl.when(jnp.logical_and(zo >= z, z >= 1))
        def _():
            z_copy(zo, 1).start()

    def forward_x(zo):
        x_copy(zo, x).start()

    def take_z(zo):
        z_copy(zo, 0).wait_recv()
        forward_z(zo)

    part = rows // 2

    def p_copy(zo, h):
        r = pl.ds(h * part, part)
        return remote(PXs.at[zo, r], PXr.at[zo, r], p_send.at[h, zo], p_recv.at[h, zo], expert=other)

    def c_copy(zo, slot, h):
        r = pl.ds(h * part, part)
        return remote(CSs.at[zo, r], CSr.at[slot, r], c_send.at[h, zo], c_recv.at[h, slot], expert=zo * nx + x)

    forward_z(z)
    forward_x(z)
    rem_w = [remote(a.at[0], b.at[1], w_send.at[i], w_recv.at[i], tensor=1 - core) for i, (a, b) in enumerate(
        ((wg_ref, Wg), (wu_ref, Wu), (wd_ref, Wd)))]
    for cp in rem_w:
        cp.start()

    table = [sorted(range(nz), key=lambda q: (abs(q - k), abs(2 * q + 1 - nz))) for k in range(nz)]

    def nth(i):
        r = table[0][i]
        for k in range(1, nz):
            r = jnp.where(z == k, table[k][i], r)
        return r

    for cp in loc_s:
        cp.wait()
    tok = tok_ref[...]
    sh = silu_mul(jnp.dot(tok, Sg[...], preferred_element_type=jnp.float32),
                  jnp.dot(tok, Su[...], preferred_element_type=jnp.float32))
    SHo[...] = jnp.dot(sh, Sd[...], preferred_element_type=jnp.float32)

    @pl.when(core == 0)
    def _():
        SHs[...] = SHo[:, half:]

    @pl.when(core == 1)
    def _():
        SHs[...] = SHo[:, :half]
    sh_copy = remote(SHs, SHr, m_send.at[0], m_recv.at[0], tensor=1 - core)
    sh_copy.start()

    for cp in loc_w:
        cp.wait()
    for cp in rem_w:
        cp.wait_recv()

    def compute(zo):
        base = zo * nx
        xs = X[pl.ds(base, nx)].reshape(nx * rows, X.shape[2])
        xin = xs[:, :width]
        O[...] = jnp.zeros_like(O)
        for hh in range(2):
            hid = silu_mul(jnp.dot(xin, Wg[hh], preferred_element_type=jnp.float32),
                           jnp.dot(xin, Wu[hh], preferred_element_type=jnp.float32))
            O[...] += jnp.dot(hid, Wd[hh], preferred_element_type=jnp.float32)
        tail = xs[:, lo:].astype(jnp.float32)
        lane = lax.broadcasted_iota(jnp.int32, tail.shape, 1) - (width - lo)
        hit = (lane == me) | (lane == me + n_all) | (lane == me + 2 * n_all)
        weight = jnp.sum(jnp.where(hit, tail, 0.0), axis=1, keepdims=True)
        O[...] = weight * O[...].astype(jnp.bfloat16).astype(jnp.float32)
        OWN[zo] = O[pl.ds(pl.multiple_of(x * rows, rows), rows), :]
        PXs[zo] = O[pl.ds(pl.multiple_of(ox * rows, rows), rows), :].astype(jnp.bfloat16)

    def column_sum(zo):
        for h in range(2):
            r = slice(h * part, (h + 1) * part)
            p_copy(zo, h).wait_recv()
            CSs[zo, r] = (OWN[zo, r] + PXr[zo, r].astype(jnp.float32)).astype(jnp.bfloat16)
            c_copy(zo, z, h).start()

    for i in range(nz):
        zi = nth(i)

        @pl.when(jnp.logical_or(z == 0, z == nz - 1))
        def _():
            if i + 1 < nz:
                take_z(nth(i + 1))
                forward_x(nth(i + 1))

        @pl.when(jnp.logical_and(z > 0, z < nz - 1))
        def _():
            if i == 0:
                for j in range(1, min(3, nz)):
                    take_z(nth(j))
                    forward_x(nth(j))
            else:
                if i + 2 < nz:
                    take_z(nth(i + 2))
                if 2 <= i < nz - 1:
                    forward_x(nth(i + 1))
        if i >= 3:
            column_sum(nth(i - 2))
        x_copy(zi, ox).wait_recv()
        compute(zi)
        if i > 0:
            for h in range(2):
                p_copy(zi, h).start()
    for h in range(2):
        p_copy(z, h).start()
    for i in range(max(1, nz - 2), nz):
        column_sum(nth(i))
    for h in range(2):
        p_copy(z, h).wait_recv()
    OWN[z] += PXr[z].astype(jnp.float32)
    for i in range(1, nz):
        zi = nth(i)
        for h in range(2):
            c_copy(zi, zi, h).wait_recv()
        OWN[z] += CSr[zi].astype(jnp.float32)

    @pl.when(core == 0)
    def _():
        FXs[...] = OWN[z, :, half:]

    @pl.when(core == 1)
    def _():
        FXs[...] = OWN[z, :, :half]
    fx_copy = remote(FXs, FXr, m_send.at[1], m_recv.at[1], tensor=1 - core)
    fx_copy.start()
    sh_copy.wait_recv()
    fx_copy.wait_recv()

    for cc in range(2):
        @pl.when(core == cc)
        def _():
            cols = slice(cc * half, (cc + 1) * half)
            for hh in range(2):
                rr = slice(hh * rows, (hh + 1) * rows)
                routed = OWN[z, :, cols] if hh == cc else FXr[...]
                total = tok_ref[rr, cols].astype(jnp.float32) + routed + (SHo[rr, cols] + SHr[rr, :])
                out_ref[rr, :] = total.astype(jnp.bfloat16)

    for cp in rem_w:
        cp.wait_send()
    sh_copy.wait_send()
    fx_copy.wait_send()
    for i in range(nz):
        zo = i

        @pl.when(jnp.logical_and(zo <= z, z + 1 < nz))
        def _():
            z_copy(zo, 0).wait_send()

        @pl.when(jnp.logical_and(zo >= z, z >= 1))
        def _():
            z_copy(zo, 1).wait_send()

        x_copy(zo, x).wait_send()
        for h in range(2):
            p_copy(zo, h).wait_send()

        @pl.when(zo != z)
        def _():
            for h in range(2):
                c_copy(zo, z, h).wait_send()


def pad(n, m):
    return -(-n // m) * m


def gather_plan(tok_count, width, expert_count, local_experts, hidden):
    if local_experts != 1 or expert_count % 2 or tok_count % 32 or width % 2:
        return None
    nz, rows = expert_count // 2, tok_count // 2
    ext = pad(width + 3 * expert_count, 128)
    if ext - width // 128 * 128 > 128:
        return None
    wide, hid, half = pad(width, 128), pad(hidden, 128), pad(width // 2, 128)
    weights = 9 * (2 * width * hid + pad(hidden, 16) * wide) * 2 // 3 + 0
    moved = expert_count * rows * ext * 2 + 4 * nz * rows * wide * 2 + nz * rows * wide * 4
    flat = tok_count * (2 * wide * 4 + 2 * half * 4 + 2 * wide * 2) + 2 * rows * half * 4
    return weights + moved + flat


def gather_local(tokens, routes, gates, w_gate, w_up, w_down, shared_gate, shared_up, shared_down):
    tok_count, width = tokens.shape
    hidden = w_gate.shape[2]
    n = lax.axis_size("expert")
    nx, nz = 2, n // 2
    rows, half = tok_count // 2, width // 2
    ext_w = pad(width + 3 * n, 128)
    bf, f32 = jnp.bfloat16, jnp.float32
    vm, dma = pltpu.VMEM, pltpu.SemaphoreType.DMA
    scratch = [
        vm((n, rows, ext_w), bf),
        vm((2, width, hidden), bf), vm((2, width, hidden), bf), vm((2, hidden, width), bf),
        vm((width, hidden), bf), vm((width, hidden), bf), vm((hidden, width), bf),
        vm((nz, rows, width), f32), vm((nx * rows, width), f32),
        vm((nz, rows, width), bf), vm((nz, rows, width), bf), vm((nz, rows, width), bf), vm((nz, rows, width), bf),
        vm((tok_count, width), f32), vm((tok_count, half), f32), vm((tok_count, half), f32),
        vm((rows, half), f32), vm((rows, half), f32),
        dma((3,)), dma((3,)), dma((3,)), dma((3,)), dma((2, nz)), dma((nz,)), dma((nz,)), dma((nz,)),
        dma((2, nz)), dma((2, nz)), dma((2, nz)), dma((2, nz)), dma((2,)), dma((2,)),
    ]
    in_vmem, in_hbm = pl.BlockSpec(memory_space=pltpu.VMEM), pl.BlockSpec(memory_space=pl.ANY)
    return pl.pallas_call(
        functools.partial(moe_kernel, nz, nx, width),
        out_shape=jax.ShapeDtypeStruct((tok_count, half), bf),
        in_specs=[in_vmem] * 3 + [in_hbm] * 6,
        out_specs=in_vmem,
        scratch_shapes=scratch,
        compiler_params=pltpu.CompilerParams(collective_id=0, has_side_effects=True, vmem_limit_bytes=60 * 1024 * 1024),
    )(tokens, routes.T, gates.T, w_gate, w_up, w_down, shared_gate, shared_up, shared_down)


def local(tokens, routes, gates, w_gate, *rest):
    need = gather_plan(*tokens.shape, lax.axis_size("expert"), w_gate.shape[0], w_gate.shape[2])
    if need is not None and lax.axis_size("tensor") == 2 and need <= VMEM_BUDGET:
        return gather_local(tokens, routes, gates, w_gate, *rest)
    return exchange_local(tokens, routes, gates, w_gate, *rest)


def solution(mesh):
    in_specs = (
        P(("groups", "expert"), None),
        P(("groups", "expert"), None),
        P(("groups", "expert"), None),
        P("expert", None, "tensor"),
        P("expert", None, "tensor"),
        P("expert", "tensor", None),
        P(None, "tensor"),
        P(None, "tensor"),
        P("tensor", None),
    )
    out_specs = P(("groups", "expert"), "tensor")
    return jax.shard_map(local, mesh=mesh, in_specs=in_specs, out_specs=out_specs, check_vma=False)
```
